32 devices in a mesh: dp: 8 (over z, y), mp: 4 (over x, core).
Axes of the slice: x: 2, y: 2, z: 4, core: 2. Of those that a mesh axis runs over, the one named last changes fastest.
Arguments:
- picture_skip_activations: bfloat16 [16384, 1152], P('dp'), as said below
- caption_closing_activations: bfloat16 [64, 1152], P('dp'), as said below
- normaliser_multipliers: float32 [3, 1152], replicated, may hold values from 0.1 to 1.9
- widening_matrix: bfloat16 [1152, 4304], P('dp', 'mp'), may hold values from -0.1875 to 0.1875
- contracting_matrix: bfloat16 [4304, 1152], P('mp', 'dp'), as said below
- caption_mapping_matrix: bfloat16 [1152, 1152], replicated, as said below
- sharpness_factor: float32 [1], replicated, may hold values from 8 to 32
- score_offset_term: float32 [1], replicated, may hold values from -8 to -3
Outputs:
- row_loss: float32 [64], P('dp')
- col_loss: float32 [64], P('dp')
The draws below stay inside these ranges and needn't reach their ends.
Inputs may be any that keep to these rules, and one draw needn't show every extreme that they name: `picture_skip_activations`: entries lie within -8 and 8. `caption_closing_activations`: entries lie within -8 and 8. `contracting_matrix`: entries are at most 4.4 / sqrt(4304) in magnitude. `caption_mapping_matrix`: diagonal entries lie within 1 - 2.1 / sqrt(1152) and 1 + 2.1 / sqrt(1152), the others within -2.1 / sqrt(1152) and 2.1 / sqrt(1152).
All inputs are finite; a program needn't handle non-finite values.
Results may differ from the reference program's by a relative error of at most 0.01.
Values may be sent and summed in bfloat16 or wider, within the bound.
A program may use at most 128 MiB of HBM per device.

```python
import math
import jax
import jax.numpy as jnp
from jax import lax

D = 1152
MLP = 4304
PATCHES = 256
IMG_DEV = 8
PAIRS = 64
N_DP = 8
N_MP = 4


latent_rank = 16


offset_amplitude = 1.5


direction_weight = 1.33


skip_spread = 0.8


head_spread = 0.7


def shared_direction(key):
    sign_table = jnp.where(jnp.arange(D) < D // 2, 1.0, -1.0).astype(jnp.float32)
    return jax.random.permutation(jax.random.fold_in(key, 101), sign_table)


def pair_offsets(key):
    latent = jax.random.normal(jax.random.fold_in(key, 202), (PAIRS, latent_rank), jnp.float32)
    basis_rows = jax.random.normal(jax.random.fold_in(key, 203), (latent_rank, D), jnp.float32) * latent_rank ** (-0.5)
    return offset_amplitude * jnp.dot(latent, basis_rows, precision=lax.Precision.HIGHEST)


def draw_picture_skip_activations(key, part):
    direction = shared_direction(key)
    offsets = pair_offsets(key)
    noise_key = jax.random.fold_in(key, 301)
    field_shape = (PAIRS, PATCHES, D)
    noise_part = jax.random.truncated_normal(noise_key, -4.5, 4.5, field_shape, jnp.float32)
    along_axis = skip_spread * jax.random.truncated_normal(jax.random.fold_in(key, 302), -3.0, 3.0, (PAIRS, PATCHES, 1), jnp.float32)
    field_sum = noise_part + offsets[:, None, :] + along_axis * direction[None, None, :]
    return jnp.clip(field_sum, -8.0, 8.0).reshape(PAIRS * PATCHES, D).astype(jnp.bfloat16)


def draw_caption_closing_activations(key, part):
    offsets = pair_offsets(key)
    noise_key = jax.random.fold_in(key, 401)
    noise_part = jax.random.truncated_normal(noise_key, -4.5, 4.5, (PAIRS, D), jnp.float32)
    return jnp.clip(noise_part + offsets, -8.0, 8.0).astype(jnp.bfloat16)


def draw_contracting_matrix(key, part):
    direction = shared_direction(key)
    sign_table = jnp.where(jnp.arange(MLP) < MLP // 2, 1.0, -1.0).astype(jnp.float32)
    unit_signs = jax.random.permutation(jax.random.fold_in(key, 501), sign_table)
    noise_key = jax.random.fold_in(key, 502)
    noise_part = jax.random.truncated_normal(noise_key, -3.0, 3.0, (MLP, D), jnp.float32)
    weights = (direction_weight * unit_signs[:, None] * direction[None, :] + noise_part) * MLP ** (-0.5)
    return weights.astype(jnp.bfloat16)


def draw_caption_mapping_matrix(key, part):
    noise_key = jax.random.fold_in(key, 601)
    noise_part = jax.random.truncated_normal(noise_key, -3.0, 3.0, (D, D), jnp.float32)
    return (jnp.eye(D, dtype=jnp.float32) + head_spread * D ** (-0.5) * noise_part).astype(jnp.bfloat16)


def steps_of(key, extent, cuts, smallest, top_value):
    gain, own = 1.0, jax.random.fold_in(key, 6)
    for position, parts in cuts:
        steps = jnp.exp(jax.random.uniform(jax.random.fold_in(own, position), (parts,), jnp.float32, smallest / len(cuts), top_value / len(cuts)))
        gain = gain * jnp.repeat(steps, extent[position] // parts).reshape([-1 if axis == position else 1 for axis in range(len(extent))])
    return gain


def bell_draw(stream_key, dims, scale, most, shards=(), kind=jnp.bfloat16):
    array = jax.random.normal(stream_key, dims, jnp.float32) * scale
    if len(shards) > 0:
        array = steps_of(stream_key, dims, shards, -0.22, 0.18) * array
    return jnp.clip(array, min=-most, max=most).astype(kind)


def setup_inputs(seed: int = 0) -> dict:
    seeds = jax.random.split(jax.random.key(seed), 9)
    return {
        "picture_skip_activations": draw_picture_skip_activations(jax.random.fold_in(seeds[8], 71), 0),
        "caption_closing_activations": draw_caption_closing_activations(jax.random.fold_in(seeds[8], 71), 0),
        "normaliser_multipliers": jnp.clip(1.0 + 0.18 * jax.random.normal(seeds[2], (3, D), jnp.float32), 0.1, 1.9),
        "widening_matrix": bell_draw(seeds[3], (D, MLP), D ** -0.5, 0.1875, ((0, 8), (1, 4))),
        "contracting_matrix": draw_contracting_matrix(jax.random.fold_in(seeds[8], 71), 0),
        "caption_mapping_matrix": draw_caption_mapping_matrix(jax.random.fold_in(seeds[8], 71), 0),
        "sharpness_factor": jnp.clip(jnp.exp(jax.random.uniform(seeds[6], (1,), jnp.float32, math.log(8.0), math.log(32.0))), 8.0, 32.0),
        "score_offset_term": jnp.clip(jax.random.uniform(seeds[7], (1,), jnp.float32, -8.0, -3.0), -8.0, -3.0),
    }


def layer_norm(values, norm_gain):
    average = lax.optimization_barrier(jnp.mean(values, axis=-1, keepdims=True))
    centred = values - average
    spread = lax.optimization_barrier(jnp.mean(centred * centred, axis=-1, keepdims=True))
    return centred * lax.rsqrt(spread + 1e-06) * norm_gain

def unit_vector(vector):
    length = jnp.sqrt(lax.optimization_barrier(jnp.sum(vector * vector, axis=-1, keepdims=True)))
    return (vector / jnp.maximum(length, 1.0)).astype(jnp.bfloat16)

def blocked_sum(image_units, contracting_matrix):
    quarter_width = MLP // N_MP
    running_sum = jnp.zeros((image_units.shape[0], contracting_matrix.shape[1]), jnp.float32)
    for quarter in range(N_MP):
        quarter_sum = jnp.dot(image_units[:, quarter * quarter_width:(quarter + 1) * quarter_width], contracting_matrix[quarter * quarter_width:(quarter + 1) * quarter_width, :], preferred_element_type=jnp.float32)
        rounded = lax.optimization_barrier(quarter_sum.astype(jnp.bfloat16))
        running_sum = running_sum + rounded.astype(jnp.float32)
    return running_sum

def reference(picture_skip_activations, caption_closing_activations, normaliser_multipliers, widening_matrix, contracting_matrix, caption_mapping_matrix, sharpness_factor, score_offset_term):

    def image_block(image_rows):
        as_float = image_rows.astype(jnp.float32)
        image_normed = layer_norm(as_float, normaliser_multipliers[0]).astype(jnp.bfloat16)
        image_units = jax.nn.gelu(jnp.dot(image_normed, widening_matrix, preferred_element_type=jnp.float32), approximate=True).astype(jnp.bfloat16)
        image_final = layer_norm(as_float + blocked_sum(image_units, contracting_matrix), normaliser_multipliers[1])
        return lax.optimization_barrier(jnp.mean(image_final.reshape(IMG_DEV, PATCHES, D), axis=1))
    grouped = picture_skip_activations.reshape(N_DP, IMG_DEV * PATCHES, D)
    image_pooled = lax.map(image_block, grouped).reshape(PAIRS, D)
    picture_code_direction = unit_vector(image_pooled)
    text_normed = layer_norm(caption_closing_activations.astype(jnp.float32), normaliser_multipliers[2]).astype(jnp.bfloat16)
    text_vector = jnp.dot(text_normed, caption_mapping_matrix, preferred_element_type=jnp.float32)
    caption_code_direction = unit_vector(text_vector)
    matching_scores = sharpness_factor[0] * jnp.dot(picture_code_direction, caption_code_direction.T, preferred_element_type=jnp.float32) + score_offset_term[0]
    labels = 2.0 * jnp.eye(PAIRS, dtype=jnp.float32) - 1.0
    loss_terms = jax.nn.softplus(-labels * matching_scores)
    return (lax.optimization_barrier(jnp.sum(loss_terms, axis=1)), lax.optimization_barrier(jnp.sum(loss_terms, axis=0)))
```

```python
import functools

import jax
import jax.numpy as jnp
from jax import lax
from jax.experimental import pallas as pl
from jax.experimental.pallas import tpu as pltpu
from jax.sharding import PartitionSpec as P

PATCHES = 256


def layer_norm(values, norm_gain):
    average = jnp.mean(values, axis=-1, keepdims=True)
    centred = values - average
    spread = jnp.mean(centred * centred, axis=-1, keepdims=True)
    return centred * lax.rsqrt(spread + 1e-06) * norm_gain


def unit_vector(vector):
    length = jnp.sqrt(jnp.sum(vector * vector, axis=-1, keepdims=True))
    return (vector / jnp.maximum(length, 1.0)).astype(jnp.bfloat16)


def pool_images(image_final):
    return jnp.mean(image_final.reshape(-1, PATCHES, image_final.shape[1]), axis=1)


def on_device(
    picture_skip_activations,
    caption_closing_activations,
    normaliser_multipliers,
    widening_matrix,
    contracting_matrix,
    caption_mapping_matrix,
    sharpness_factor,
    score_offset_term,
):
    image_rows = picture_skip_activations.astype(jnp.float32)
    image_normed = layer_norm(image_rows, normaliser_multipliers[0]).astype(jnp.bfloat16)
    inner_weight = lax.all_gather(widening_matrix, "dp", axis=0, tiled=True)
    image_units = jax.nn.gelu(
        jnp.dot(image_normed, inner_weight, preferred_element_type=jnp.float32), approximate=True
    ).astype(jnp.bfloat16)
    partial_out = jnp.dot(
        image_units,
        lax.all_gather(contracting_matrix, "dp", axis=1, tiled=True),
        preferred_element_type=jnp.float32,
    )
    unit_share = lax.psum_scatter(
        partial_out.astype(jnp.bfloat16), "mp", scatter_dimension=0, tiled=True
    ).astype(jnp.float32)
    own_count = unit_share.shape[0]
    own_first = lax.axis_index("mp") * own_count
    own_rows = lax.dynamic_slice_in_dim(image_rows, own_first, own_count, 0)
    image_final = layer_norm(own_rows + unit_share, normaliser_multipliers[1])
    own_emb = unit_vector(pool_images(image_final))
    picture_code_direction = lax.all_gather(own_emb, "mp", axis=0, tiled=True)
    text_normed = layer_norm(
        caption_closing_activations.astype(jnp.float32), normaliser_multipliers[2]
    ).astype(jnp.bfloat16)
    text_vector = jnp.dot(text_normed, caption_mapping_matrix, preferred_element_type=jnp.float32)
    caption_code_direction = unit_vector(text_vector)
    offset = lax.axis_index("dp") * picture_code_direction.shape[0]
    matching_scores = (
        sharpness_factor[0]
        * jnp.einsum(
            "pe,qe->pq",
            picture_code_direction,
            lax.all_gather(caption_code_direction, "dp", axis=0, tiled=True),
            preferred_element_type=jnp.float32,
        )
        + score_offset_term[0]
    )
    row_index = offset + lax.broadcasted_iota(jnp.int32, matching_scores.shape, 0)
    col_index = lax.broadcasted_iota(jnp.int32, matching_scores.shape, 1)
    labels = jnp.where(row_index == col_index, 1.0, -1.0).astype(jnp.float32)
    loss_terms = jax.nn.softplus(-labels * matching_scores)
    row_loss = jnp.sum(loss_terms, axis=1)
    col_loss = lax.psum_scatter(jnp.sum(loss_terms, axis=0), "dp", scatter_dimension=0, tiled=True)
    return (row_loss, col_loss)


MESH = pl.DeviceIdType.MESH
ROW_TILE = 256
LANES = 128


def dot_nt(a, b):
    return lax.dot_general(a, b, (((1,), (1,)), ((), ())), preferred_element_type=jnp.float32)


def fused_kernel(
    n_dp,
    n_mp,
    x_hbm,
    text_ref,
    gain_ref,
    w1_own,
    w2_own,
    map_hbm,
    sharp_ref,
    offset_ref,
    out_ref,
    x_buf,
    xn_buf,
    map_buf,
    w1_full,
    w2_full,
    units,
    partial,
    core_in,
    cross_out,
    cross_in,
    final,
    texts,
    message,
    slots,
    local_sem,
    y_send,
    z_send,
    w_recv,
    text_send,
    text_recv,
    core_send,
    core_recv,
    cross_send,
    cross_recv,
    msg_send,
    msg_recv,
):
    dp = lax.axis_index("dp")
    mp = lax.axis_index("mp")
    n_all = n_dp * n_mp
    me = dp * n_mp + mp
    rows, width = x_buf.shape
    block = w1_own.shape[0]
    own_rows = rows // n_mp
    own_images = own_rows // PATCHES
    dev_images = rows // PATCHES
    dev_texts = text_ref.shape[0]
    pairs = n_dp * dev_texts
    tiles = rows // ROW_TILE
    nz = n_dp // 2
    z, y = lax.div(dp, 2), lax.rem(dp, 2)
    y_peer = dp + 1 - 2 * y
    core = lax.rem(mp, 2)
    sibling = mp + 1 - 2 * core
    across = lax.rem(mp + 2, n_mp)
    pair = 2 * block

    shorter = jnp.minimum(z, nz - 1 - z)
    toward = jnp.where(z < nz - 1 - z, 1, -1)
    order, sides = [z], [None]
    for j in range(1, nz):
        sign = jnp.where(j <= 2 * shorter, 1 if j % 2 else -1, toward)
        hop = jnp.where(j <= 2 * shorter, (j + 1) // 2, j - shorter)
        order.append(z + sign * hop)
        sides.append(sign)

    x_copy = pltpu.make_async_copy(x_hbm, x_buf, local_sem.at[0])
    map_copy = pltpu.make_async_copy(map_hbm, map_buf, local_sem.at[1])
    x_copy.start()
    map_copy.start()

    barrier = pltpu.get_barrier_semaphore()

    def greet(k, carry):
        peer = lax.rem(me + k, n_all)
        pl.semaphore_signal(
            barrier, inc=1, device_id=(lax.div(peer, n_mp), lax.rem(peer, n_mp)), device_id_type=MESH
        )
        return carry

    lax.fori_loop(1, n_all, greet, 0)

    full = (w1_full, w2_full)
    own = (w1_own, w2_own)

    def span(d):
        return pl.ds(pl.multiple_of(d * block, block), block)

    def weight_copy(w, d, is_own, target, send_sem):
        return pltpu.make_async_remote_copy(
            src_ref=own[w] if is_own else full[w].at[span(d)],
            dst_ref=full[w].at[span(d)],
            send_sem=send_sem,
            recv_sem=w_recv.at[w, d],
            device_id=(target, mp),
            device_id_type=MESH,
        )

    def y_copy(w, j):
        return weight_copy(w, 2 * order[j] + y, j == 0, y_peer, y_send.at[w, j])

    def own_z_copy(w, sign):
        return weight_copy(w, dp, True, dp + 2 * sign, z_send.at[w, 0 if sign > 0 else nz])

    def pass_on_copy(w, j):
        return weight_copy(w, 2 * order[j] + y, False, dp - 2 * sides[j], z_send.at[w, j])

    def can_pass(j):
        there = z - sides[j]
        return jnp.logical_and(there >= 0, there < nz)

    def start_own(w):
        @pl.when(z + 1 < nz)
        def _():
            own_z_copy(w, 1).start()

        @pl.when(z >= 1)
        def _():
            own_z_copy(w, -1).start()

        y_copy(w, 0).start()

    def wait_block(w, d):
        pltpu.make_async_copy(own[w], full[w].at[span(d)], w_recv.at[w, d]).wait()

    def pass_on(w, j):
        wait_block(w, 2 * order[j] + y)

        @pl.when(can_pass(j))
        def _():
            pass_on_copy(w, j).start()

        y_copy(w, j).start()

    pl.semaphore_wait(barrier, n_all - 1)
    start_own(0)

    w1_full[span(dp), :] = w1_own[...]
    w2_full[span(dp), :] = w2_own[...]

    map_copy.wait()
    text_normed = layer_norm(text_ref[...].astype(jnp.float32), gain_ref[2:3, :]).astype(jnp.bfloat16)
    text_vector = jnp.dot(text_normed, map_buf[...], preferred_element_type=jnp.float32)
    texts[dp] = unit_vector(text_vector)

    def text_copy(k):
        return pltpu.make_async_remote_copy(
            src_ref=texts.at[dp],
            dst_ref=texts.at[dp],
            send_sem=text_send.at[k],
            recv_sem=text_recv.at[k],
            device_id=(lax.rem(dp + k, n_dp), mp),
            device_id_type=MESH,
        )

    for k in range(1, n_dp):
        text_copy(k).start()

    x_copy.wait()

    def normalise(t, carry):
        r = pl.ds(pl.multiple_of(t * ROW_TILE, ROW_TILE), ROW_TILE)
        xn_buf[r, :] = layer_norm(x_buf[r, :].astype(jnp.float32), gain_ref[0:1, :]).astype(jnp.bfloat16)
        return carry

    lax.fori_loop(0, tiles // 2, normalise, 0)
    pass_on(0, 1)
    lax.fori_loop(tiles // 2, tiles, normalise, 0)
    for j in range(2, nz):
        pass_on(0, j)
    start_own(1)

    for t in range(own_rows // ROW_TILE):
        r = pl.ds(pl.multiple_of(mp * own_rows + t * ROW_TILE, ROW_TILE), ROW_TILE)
        final[:, t * ROW_TILE : (t + 1) * ROW_TILE] = x_buf[r, :].astype(jnp.float32).T

    for j in range(nz):
        wait_block(0, 2 * order[j] + 1 - y)

    def widen(t, carry):
        r = pl.ds(pl.multiple_of(t * ROW_TILE, ROW_TILE), ROW_TILE)
        hidden = jnp.dot(xn_buf[r, :], w1_full[...], preferred_element_type=jnp.float32)
        units[r, :] = jax.nn.gelu(hidden, approximate=True).astype(jnp.bfloat16)
        return carry

    lax.fori_loop(0, tiles // 2, widen, 0)
    pass_on(1, 1)
    lax.fori_loop(tiles // 2, tiles, widen, 0)

    def group(j):
        return pl.ds(pl.multiple_of(order[j] * pair, pair), pair)

    def quarter(q):
        return pl.ds(pl.multiple_of(q * own_rows, own_rows), own_rows)

    sides_x = n_mp // 2
    my_side = lax.div(mp, 2)

    def core_copy(j, s):
        return pltpu.make_async_remote_copy(
            src_ref=partial.at[group(j), quarter(2 * s + 1 - core)],
            dst_ref=core_in.at[group(j), pl.ds(s * own_rows, own_rows)],
            send_sem=core_send.at[j, s],
            recv_sem=core_recv.at[j, s],
            device_id=(dp, sibling),
            device_id_type=MESH,
        )

    def cross_copy(j):
        return pltpu.make_async_remote_copy(
            src_ref=cross_out.at[group(j)],
            dst_ref=cross_in.at[group(j)],
            send_sem=cross_send.at[j],
            recv_sem=cross_recv.at[j],
            device_id=(dp, across),
            device_id_type=MESH,
        )

    def contract(j):
        wait_block(1, 2 * order[j] + 1 - y)
        weight = w2_full[group(j), :]
        for t in range(n_mp):
            r = pl.ds(t * own_rows, own_rows)
            partial[group(j), r] = dot_nt(weight, units[r, :]).astype(jnp.bfloat16)
        for s in range(sides_x):
            core_copy(j, s).start()

    def meet(j):
        for s in range(sides_x):
            core_copy(j, s).wait_recv()
        g = group(j)
        there = lax.rem(my_side + 1, sides_x)
        summed = partial[g, quarter(across)].astype(jnp.float32) + core_in[g, quarter(there)].astype(jnp.float32)
        cross_out[g, :] = summed.astype(jnp.bfloat16)
        cross_copy(j).start()
        final[g, :] = (
            final[g, :]
            + partial[g, quarter(mp)].astype(jnp.float32)
            + core_in[g, quarter(my_side)].astype(jnp.float32)
        )

    for j in range(nz):
        if j + 1 < nz and j >= 1:
            pass_on(1, j + 1)
        contract(j)
        if j == 0 and nz > 2:
            pass
        if j >= 1:
            meet(j - 1)
    meet(nz - 1)

    for j in range(nz):
        cross_copy(j).wait_recv()
        final[group(j), :] = final[group(j), :] + cross_in[group(j), :].astype(jnp.float32)

    value = final[...]
    average = jnp.mean(value, axis=0, keepdims=True)
    centred = value - average
    spread = jnp.mean(centred * centred, axis=0, keepdims=True)
    scaled = centred * lax.rsqrt(spread + 1e-06)
    pooled = jnp.zeros((8, width), jnp.float32)
    row_place = lax.broadcasted_iota(jnp.int32, (8, width), 0)
    for image in range(own_images):
        folded = jnp.zeros((width, LANES), jnp.float32)
        for c in range(PATCHES // LANES):
            first = image * PATCHES + c * LANES
            folded = folded + scaled[:, first : first + LANES]
        one = jnp.sum(folded.T, axis=0, keepdims=True) * (1.0 / PATCHES)
        pooled = jnp.where(row_place == image, one, pooled)
    image_emb = unit_vector(pooled * gain_ref[1:2, :])

    for k in range(1, n_dp):
        text_copy(k).wait_recv()
    every_text = texts[...].astype(jnp.float32).reshape(pairs, width)
    every_text = jnp.concatenate([every_text, jnp.zeros((LANES - pairs, width), jnp.float32)], axis=0)
    scores = sharp_ref[0] * dot_nt(image_emb, every_text.astype(jnp.bfloat16)) + offset_ref[0]
    row = lax.broadcasted_iota(jnp.int32, scores.shape, 0)
    col = lax.broadcasted_iota(jnp.int32, scores.shape, 1)
    own_row = row < own_images
    matching = row + dp * dev_images + mp * own_images == col
    signed = jnp.where(matching, -scores, scores)
    terms = jnp.maximum(signed, 0.0) + jnp.log1p(jnp.exp(-jnp.abs(signed)))
    terms = jnp.where(jnp.logical_and(own_row, col < pairs), terms, 0.0)
    row_sum = jnp.sum(terms, axis=1, keepdims=True)
    terms = terms + jnp.where(jnp.logical_and(own_row, col == pairs + row), row_sum, 0.0)
    sent = jnp.sum(terms, axis=0, keepdims=True)
    message[...] = sent
    slots[me] = sent

    def msg_copy(k):
        peer = lax.rem(me + k, n_all)
        return pltpu.make_async_remote_copy(
            src_ref=message,
            dst_ref=slots.at[me],
            send_sem=msg_send.at[k],
            recv_sem=msg_recv.at[k],
            device_id=(lax.div(peer, n_mp), lax.rem(peer, n_mp)),
            device_id_type=MESH,
        )

    def send_msg(k, carry):
        msg_copy(k).start()
        return carry

    lax.fori_loop(1, n_all, send_msg, 0)

    for w in range(2):
        @pl.when(z + 1 < nz)
        def _():
            own_z_copy(w, 1).wait_send()

        @pl.when(z >= 1)
        def _():
            own_z_copy(w, -1).wait_send()

        for j in range(nz):
            y_copy(w, j).wait_send()
            if j >= 1:

                @pl.when(can_pass(j))
                def _():
                    pass_on_copy(w, j).wait_send()

    for k in range(1, n_dp):
        text_copy(k).wait_send()
    for j in range(nz):
        for s in range(sides_x):
            core_copy(j, s).wait_send()
        cross_copy(j).wait_send()

    def end_msg(k, carry):
        msg_copy(k).wait()
        return carry

    lax.fori_loop(1, n_all, end_msg, 0)

    total = jnp.zeros((1, LANES), jnp.float32)
    for s in range(n_all):
        total = total + slots[s]
    lane = lax.broadcasted_iota(jnp.int32, (1, LANES), 1)
    place = lax.broadcasted_iota(jnp.int32, (dev_texts, LANES), 0)
    wide = lax.broadcasted_iota(jnp.int32, (dev_texts, LANES), 1)
    picked = jnp.where(wide == dp * dev_texts + place, jnp.broadcast_to(total, wide.shape), 0.0)
    col_own = jnp.sum(picked, axis=1, keepdims=True)
    place_r = lax.broadcasted_iota(jnp.int32, (dev_images, LANES), 0)
    wide_r = lax.broadcasted_iota(jnp.int32, (dev_images, LANES), 1)
    row_own = jnp.zeros((dev_images, 1), jnp.float32)
    for m in range(n_mp):
        theirs = jnp.broadcast_to(slots[dp * n_mp + m], wide_r.shape)
        mine = jnp.logical_and(
            wide_r - pairs == place_r - m * own_images,
            jnp.logical_and(wide_r >= pairs, wide_r < pairs + own_images),
        )
        row_own = row_own + jnp.sum(jnp.where(mine, theirs, 0.0), axis=1, keepdims=True)
    out_ref[...] = jnp.where(wide == 0, row_own, col_own)


def fused(
    n_dp,
    n_mp,
    picture_skip_activations,
    caption_closing_activations,
    normaliser_multipliers,
    widening_matrix,
    contracting_matrix,
    caption_mapping_matrix,
    sharpness_factor,
    score_offset_term,
):
    rows, width = picture_skip_activations.shape
    block, hidden = widening_matrix.shape
    extra = -hidden % LANES
    hidden += extra
    w1 = jnp.pad(widening_matrix, ((0, 0), (0, extra)))
    w2 = jnp.pad(contracting_matrix, ((0, extra), (0, 0))).T
    own_rows = rows // n_mp
    nz, sides_x, n_all = n_dp // 2, n_mp // 2, n_dp * n_mp
    dev_texts = caption_closing_activations.shape[0]
    bf16, f32 = jnp.bfloat16, jnp.float32
    vmem = pl.BlockSpec(memory_space=pltpu.VMEM)
    hbm = pl.BlockSpec(memory_space=pl.ANY)
    smem = pl.BlockSpec(memory_space=pltpu.SMEM)
    dma = pltpu.SemaphoreType.DMA
    out = pl.pallas_call(
        functools.partial(fused_kernel, n_dp, n_mp),
        out_shape=jax.ShapeDtypeStruct((dev_texts, LANES), f32),
        in_specs=[hbm, vmem, vmem, vmem, vmem, hbm, smem, smem],
        out_specs=vmem,
        scratch_shapes=[
            pltpu.VMEM((rows, width), bf16),
            pltpu.VMEM((rows, width), bf16),
            pltpu.VMEM((width, width), bf16),
            pltpu.VMEM((width, hidden), bf16),
            pltpu.VMEM((width, hidden), bf16),
            pltpu.VMEM((rows, hidden), bf16),
            pltpu.VMEM((width, rows), bf16),
            pltpu.VMEM((width, sides_x * own_rows), bf16),
            pltpu.VMEM((width, own_rows), bf16),
            pltpu.VMEM((width, own_rows), bf16),
            pltpu.VMEM((width, own_rows), f32),
            pltpu.VMEM((n_dp, dev_texts, width), bf16),
            pltpu.VMEM((1, LANES), f32),
            pltpu.VMEM((n_all, 1, LANES), f32),
            dma((2,)),
            dma((2, nz)),
            dma((2, nz + 1)),
            dma((2, n_dp)),
            dma((n_dp,)),
            dma((n_dp,)),
            dma((nz, sides_x)),
            dma((nz, sides_x)),
            dma((nz,)),
            dma((nz,)),
            dma((n_all,)),
            dma((n_all,)),
        ],
        compiler_params=pltpu.CompilerParams(
            collective_id=0, has_side_effects=True, vmem_limit_bytes=60 * 1024 * 1024
        ),
    )(
        picture_skip_activations,
        caption_closing_activations,
        normaliser_multipliers,
        w1,
        w2,
        caption_mapping_matrix,
        sharpness_factor,
        score_offset_term,
    )
    return out[:, 0], out[:, 1]


def pick(n_dp, n_mp, *args):
    pictures, captions, _, widening = args[:4]
    rows, width = pictures.shape
    pairs = captions.shape[0] * n_dp
    fits = (
        n_dp % 2 == 0
        and n_dp >= 4
        and n_mp == 4
        and widening.shape[0] % 16 == 0
        and rows % (n_mp * PATCHES) == 0
        and width % LANES == 0
        and rows // PATCHES == captions.shape[0]
        and captions.shape[0] % 8 == 0
        and pairs + rows // (n_mp * PATCHES) <= LANES
    )
    return fused(n_dp, n_mp, *args) if fits else on_device(*args)


def solution(mesh):
    return jax.shard_map(
        functools.partial(pick, mesh.shape["dp"], mesh.shape["mp"]),
        mesh=mesh,
        in_specs=(P("dp", None), P("dp", None), P(), P("dp", "mp"), P("mp", "dp"), P(), P(), P()),
        out_specs=(P("dp"), P("dp")),
        check_vma=False,
    )
```

```python
import functools

import jax
import jax.numpy as jnp
from jax import lax
from jax.experimental import pallas as pl
from jax.experimental.pallas import tpu as pltpu
from jax.sharding import PartitionSpec as P

PATCHES = 256


def layer_norm(values, norm_gain):
    average = jnp.mean(values, axis=-1, keepdims=True)
    centred = values - average
    spread = jnp.mean(centred * centred, axis=-1, keepdims=True)
    return centred * lax.rsqrt(spread + 1e-06) * norm_gain


def unit_vector(vector):
    length = jnp.sqrt(jnp.sum(vector * vector, axis=-1, keepdims=True))
    return (vector / jnp.maximum(length, 1.0)).astype(jnp.bfloat16)


def pool_images(image_final):
    return jnp.mean(image_final.reshape(-1, PATCHES, image_final.shape[1]), axis=1)


def on_device(
    picture_skip_activations,
    caption_closing_activations,
    normaliser_multipliers,
    widening_matrix,
    contracting_matrix,
    caption_mapping_matrix,
    sharpness_factor,
    score_offset_term,
):
    image_rows = picture_skip_activations.astype(jnp.float32)
    image_normed = layer_norm(image_rows, normaliser_multipliers[0]).astype(jnp.bfloat16)
    inner_weight = lax.all_gather(widening_matrix, "dp", axis=0, tiled=True)
    image_units = jax.nn.gelu(
        jnp.dot(image_normed, inner_weight, preferred_element_type=jnp.float32), approximate=True
    ).astype(jnp.bfloat16)
    partial_out = jnp.dot(
        image_units,
        lax.all_gather(contracting_matrix, "dp", axis=1, tiled=True),
        preferred_element_type=jnp.float32,
    )
    unit_share = lax.psum_scatter(
        partial_out.astype(jnp.bfloat16), "mp", scatter_dimension=0, tiled=True
    ).astype(jnp.float32)
    own_count = unit_share.shape[0]
    own_first = lax.axis_index("mp") * own_count
    own_rows = lax.dynamic_slice_in_dim(image_rows, own_first, own_count, 0)
    image_final = layer_norm(own_rows + unit_share, normaliser_multipliers[1])
    own_emb = unit_vector(pool_images(image_final))
    picture_code_direction = lax.all_gather(own_emb, "mp", axis=0, tiled=True)
    text_normed = layer_norm(
        caption_closing_activations.astype(jnp.float32), normaliser_multipliers[2]
    ).astype(jnp.bfloat16)
    text_vector = jnp.dot(text_normed, caption_mapping_matrix, preferred_element_type=jnp.float32)
    caption_code_direction = unit_vector(text_vector)
    offset = lax.axis_index("dp") * picture_code_direction.shape[0]
    matching_scores = (
        sharpness_factor[0]
        * jnp.einsum(
            "pe,qe->pq",
            picture_code_direction,
            lax.all_gather(caption_code_direction, "dp", axis=0, tiled=True),
            preferred_element_type=jnp.float32,
        )
        + score_offset_term[0]
    )
    row_index = offset + lax.broadcasted_iota(jnp.int32, matching_scores.shape, 0)
    col_index = lax.broadcasted_iota(jnp.int32, matching_scores.shape, 1)
    labels = jnp.where(row_index == col_index, 1.0, -1.0).astype(jnp.float32)
    loss_terms = jax.nn.softplus(-labels * matching_scores)
    row_loss = jnp.sum(loss_terms, axis=1)
    col_loss = lax.psum_scatter(jnp.sum(loss_terms, axis=0), "dp", scatter_dimension=0, tiled=True)
    return (row_loss, col_loss)


MESH = pl.DeviceIdType.MESH
ROW_TILE = 256
LANES = 128


def dot_nt(a, b):
    return lax.dot_general(a, b, (((1,), (1,)), ((), ())), preferred_element_type=jnp.float32)


def fused_kernel(
    n_dp,
    n_mp,
    x_hbm,
    text_ref,
    gain_ref,
    w1_own,
    w2_own,
    map_hbm,
    sharp_ref,
    offset_ref,
    out_ref,
    x_buf,
    xn_buf,
    map_buf,
    w1_full,
    w2_full,
    units,
    partial,
    core_in,
    cross_out,
    cross_in,
    final,
    texts,
    message,
    slots,
    local_sem,
    y_send,
    z_send,
    w_recv,
    core_send,
    core_recv,
    cross_send,
    cross_recv,
    msg_send,
    msg_recv,
):
    dp = lax.axis_index("dp")
    mp = lax.axis_index("mp")
    n_all = n_dp * n_mp
    me = dp * n_mp + mp
    rows, width = x_buf.shape
    block = w1_own.shape[0]
    own_rows = rows // n_mp
    own_images = own_rows // PATCHES
    dev_images = rows // PATCHES
    dev_texts = text_ref.shape[0]
    pairs = n_dp * dev_texts
    tiles = rows // ROW_TILE
    nz = n_dp // 2
    z, y = lax.div(dp, 2), lax.rem(dp, 2)
    y_peer = dp + 1 - 2 * y
    core = lax.rem(mp, 2)
    sibling = mp + 1 - 2 * core
    across = lax.rem(mp + 2, n_mp)
    pair = 2 * block

    shorter = jnp.minimum(z, nz - 1 - z)
    toward = jnp.where(z < nz - 1 - z, 1, -1)
    order, sides = [z], [None]
    for j in range(1, nz):
        sign = jnp.where(j <= 2 * shorter, 1 if j % 2 else -1, toward)
        hop = jnp.where(j <= 2 * shorter, (j + 1) // 2, j - shorter)
        order.append(z + sign * hop)
        sides.append(sign)

    x_copy = pltpu.make_async_copy(x_hbm, x_buf, local_sem.at[0])
    map_copy = pltpu.make_async_copy(map_hbm, map_buf, local_sem.at[1])
    x_copy.start()
    map_copy.start()

    barrier = pltpu.get_barrier_semaphore()

    def greet(k, carry):
        peer = lax.rem(me + k, n_all)
        pl.semaphore_signal(
            barrier, inc=1, device_id=(lax.div(peer, n_mp), lax.rem(peer, n_mp)), device_id_type=MESH
        )
        return carry

    lax.fori_loop(1, n_all, greet, 0)

    pieces = next(c for c in (3, 2, 1) if block % (16 * c) == 0)
    piece = block // pieces
    counts = (pieces, pieces, 1)

    def own_part(w, c):
        if w == 2:
            return texts.at[dp]
        return (w1_own, w2_own)[w].at[pl.ds(c * piece, piece)]

    def part(w, d, c):
        if w == 2:
            return texts.at[d]
        return (w1_full, w2_full)[w].at[pl.ds(pl.multiple_of(d * block + c * piece, 16), piece)]

    def gather_copy(w, d, c, is_own, target, send_sem):
        return pltpu.make_async_remote_copy(
            src_ref=own_part(w, c) if is_own else part(w, d, c),
            dst_ref=part(w, d, c),
            send_sem=send_sem,
            recv_sem=w_recv.at[w, d, c],
            device_id=(target, mp),
            device_id_type=MESH,
        )

    def y_copy(w, j, c):
        return gather_copy(w, 2 * order[j] + y, c, j == 0, y_peer, y_send.at[w, j, c])

    def own_z_copy(w, sign, c):
        return gather_copy(w, dp, c, True, dp + 2 * sign, z_send.at[w, 0 if sign > 0 else nz, c])

    def pass_on_copy(w, j, c):
        return gather_copy(w, 2 * order[j] + y, c, False, dp - 2 * sides[j], z_send.at[w, j, c])

    def can_pass(j):
        there = z - sides[j]
        return jnp.logical_and(there >= 0, there < nz)

    def start_z(w, sign):
        for c in range(counts[w]):
            own_z_copy(w, sign, c).start()

    def start_y(w, j):
        for c in range(counts[w]):
            y_copy(w, j, c).start()

    def start_own(w):
        @pl.when(z + 1 < nz)
        def _():
            start_z(w, 1)

        @pl.when(z >= 1)
        def _():
            start_z(w, -1)

        start_y(w, 0)

    def wait_part(w, d, c):
        pltpu.make_async_copy(own_part(w, c), part(w, d, c), w_recv.at[w, d, c]).wait()

    def wait_block(w, d):
        for c in range(counts[w]):
            wait_part(w, d, c)

    def pass_on(w, j):
        for c in range(counts[w]):
            wait_part(w, 2 * order[j] + y, c)

            @pl.when(can_pass(j))
            def _():
                pass_on_copy(w, j, c).start()

            y_copy(w, j, c).start()

    with jax.named_scope("barrier"):
        pl.semaphore_wait(barrier, n_all - 1)
    start_own(0)

    w1_full[pl.ds(pl.multiple_of(dp * block, block), block), :] = w1_own[...]
    w2_full[pl.ds(pl.multiple_of(dp * block, block), block), :] = w2_own[...]

    with jax.named_scope("mapwait"):
        map_copy.wait()
    text_normed = layer_norm(text_ref[...].astype(jnp.float32), gain_ref[2:3, :]).astype(jnp.bfloat16)
    text_vector = jnp.dot(text_normed, map_buf[...], preferred_element_type=jnp.float32)
    texts[dp] = unit_vector(text_vector)

    start_own(2)

    @pl.when(z == 0)
    def _():
        start_z(1, 1)

    @pl.when(z == nz - 1)
    def _():
        start_z(1, -1)

    with jax.named_scope("xwait"):
        x_copy.wait()

    def normalise(t, carry):
        r = pl.ds(pl.multiple_of(t * ROW_TILE, ROW_TILE), ROW_TILE)
        xn_buf[r, :] = layer_norm(x_buf[r, :].astype(jnp.float32), gain_ref[0:1, :]).astype(jnp.bfloat16)
        return carry

    with jax.named_scope("ln0"):
        lax.fori_loop(0, tiles // 2, normalise, 0)
    def pass_first(j):
        with jax.named_scope(f"pass_w1_{j}"):
            pass_on(0, j)
        with jax.named_scope(f"pass_text_{j}"):
            pass_on(2, j)

        @pl.when(jnp.logical_and(order[j] == 0, z + 1 < nz))
        def _():
            start_z(1, 1)

        @pl.when(jnp.logical_and(order[j] == nz - 1, z >= 1))
        def _():
            start_z(1, -1)

    pass_first(1)
    with jax.named_scope("ln1"):
        lax.fori_loop(tiles // 2, tiles, normalise, 0)
    for j in range(2, nz):
        pass_first(j)
    start_y(1, 0)

    for t in range(own_rows // ROW_TILE):
        r = pl.ds(pl.multiple_of(mp * own_rows + t * ROW_TILE, ROW_TILE), ROW_TILE)
        final[:, t * ROW_TILE : (t + 1) * ROW_TILE] = x_buf[r, :].astype(jnp.float32).T

    for j in range(nz - 1):
        with jax.named_scope(f"wait_w1y_{j}"):
            wait_block(0, 2 * order[j] + 1 - y)
    with jax.named_scope("pass_w2_1"):
        pass_on(1, 1)
    with jax.named_scope("wait_w1y_last"):
        wait_block(0, 2 * order[nz - 1] + 1 - y)

    def widen(t, carry):
        r = pl.ds(pl.multiple_of(t * ROW_TILE, ROW_TILE), ROW_TILE)
        hidden = jnp.dot(xn_buf[r, :], w1_full[...], preferred_element_type=jnp.float32)
        units[r, :] = jax.nn.gelu(hidden, approximate=True).astype(jnp.bfloat16)
        return carry

    with jax.named_scope("widen0"):
        lax.fori_loop(0, tiles // 2, widen, 0)
    if nz > 2:
        with jax.named_scope("pass_w2_2"):
            pass_on(1, 2)
    with jax.named_scope("widen1"):
        lax.fori_loop(tiles // 2, tiles, widen, 0)

    def group(j):
        if j < nz - 1:
            return pl.ds(pl.multiple_of(order[j] * pair, pair), pair)
        side = y if j == nz - 1 else 1 - y
        return pl.ds(pl.multiple_of((2 * order[nz - 1] + side) * block, block), block)

    def quarter(q):
        return pl.ds(pl.multiple_of(q * own_rows, own_rows), own_rows)

    sides_x = n_mp // 2
    my_side = lax.div(mp, 2)

    def core_copy(j, s):
        return pltpu.make_async_remote_copy(
            src_ref=partial.at[group(j), quarter(2 * s + 1 - core)],
            dst_ref=core_in.at[group(j), pl.ds(s * own_rows, own_rows)],
            send_sem=core_send.at[j, s],
            recv_sem=core_recv.at[j, s],
            device_id=(dp, sibling),
            device_id_type=MESH,
        )

    def cross_copy(j):
        return pltpu.make_async_remote_copy(
            src_ref=cross_out.at[group(j)],
            dst_ref=cross_in.at[group(j)],
            send_sem=cross_send.at[j],
            recv_sem=cross_recv.at[j],
            device_id=(dp, across),
            device_id_type=MESH,
        )

    def contract(j):
        if j != nz - 1:
            with jax.named_scope(f"wait_w2y_{j}"):
                wait_block(1, 2 * order[min(j, nz - 1)] + 1 - y)
        weight = w2_full[group(j), :]
        for t in range(n_mp):
            r = pl.ds(t * own_rows, own_rows)
            partial[group(j), r] = dot_nt(weight, units[r, :]).astype(jnp.bfloat16)
        for s in range(sides_x):
            core_copy(j, s).start()

    def meet(j):
        for s in range(sides_x):
            core_copy(j, s).wait_recv()
        g = group(j)
        there = lax.rem(my_side + 1, sides_x)
        summed = partial[g, quarter(across)].astype(jnp.float32) + core_in[g, quarter(there)].astype(jnp.float32)
        cross_out[g, :] = summed.astype(jnp.bfloat16)
        cross_copy(j).start()
        final[g, :] = (
            final[g, :]
            + partial[g, quarter(mp)].astype(jnp.float32)
            + core_in[g, quarter(my_side)].astype(jnp.float32)
        )

    for j in range(3, nz):
        with jax.named_scope(f"pass_w2_{j}"):
            pass_on(1, j)
    for j in range(nz + 1):
        contract(j)
        with jax.named_scope(f"meet_{j}"):
            meet(j)

    for j in range(nz + 1):
        with jax.named_scope(f"wait_x_{j}"):
            cross_copy(j).wait_recv()
        final[group(j), :] = final[group(j), :] + cross_in[group(j), :].astype(jnp.float32)

    value = final[...]
    average = jnp.mean(value, axis=0, keepdims=True)
    centred = value - average
    spread = jnp.mean(centred * centred, axis=0, keepdims=True)
    scaled = centred * lax.rsqrt(spread + 1e-06)
    pooled = jnp.zeros((8, width), jnp.float32)
    row_place = lax.broadcasted_iota(jnp.int32, (8, width), 0)
    for image in range(own_images):
        folded = jnp.zeros((width, LANES), jnp.float32)
        for c in range(PATCHES // LANES):
            first = image * PATCHES + c * LANES
            folded = folded + scaled[:, first : first + LANES]
        one = jnp.sum(folded.T, axis=0, keepdims=True) * (1.0 / PATCHES)
        pooled = jnp.where(row_place == image, one, pooled)
    image_emb = unit_vector(pooled * gain_ref[1:2, :])

    for j in range(nz):
        wait_block(2, 2 * order[j] + 1 - y)
    every_text = texts[...].astype(jnp.float32).reshape(pairs, width)
    every_text = jnp.concatenate([every_text, jnp.zeros((LANES - pairs, width), jnp.float32)], axis=0)
    scores = sharp_ref[0] * dot_nt(image_emb, every_text.astype(jnp.bfloat16)) + offset_ref[0]
    row = lax.broadcasted_iota(jnp.int32, scores.shape, 0)
    col = lax.broadcasted_iota(jnp.int32, scores.shape, 1)
    own_row = row < own_images
    matching = row + dp * dev_images + mp * own_images == col
    signed = jnp.where(matching, -scores, scores)
    terms = jnp.maximum(signed, 0.0) + jnp.log1p(jnp.exp(-jnp.abs(signed)))
    terms = jnp.where(jnp.logical_and(own_row, col < pairs), terms, 0.0)
    row_sum = jnp.sum(terms, axis=1, keepdims=True)
    terms = terms + jnp.where(jnp.logical_and(own_row, col == pairs + row), row_sum, 0.0)
    sent = jnp.sum(terms, axis=0, keepdims=True)
    message[...] = sent
    slots[me] = sent

    def msg_copy(k):
        peer = lax.rem(me + k, n_all)
        return pltpu.make_async_remote_copy(
            src_ref=message,
            dst_ref=slots.at[me],
            send_sem=msg_send.at[k],
            recv_sem=msg_recv.at[k],
            device_id=(lax.div(peer, n_mp), lax.rem(peer, n_mp)),
            device_id_type=MESH,
        )

    def send_msg(k, carry):
        msg_copy(k).start()
        return carry

    lax.fori_loop(1, n_all, send_msg, 0)

    for w in range(3):
        for c in range(counts[w]):

            @pl.when(z + 1 < nz)
            def _():
                own_z_copy(w, 1, c).wait_send()

            @pl.when(z >= 1)
            def _():
                own_z_copy(w, -1, c).wait_send()

            for j in range(nz):
                y_copy(w, j, c).wait_send()
                if j >= 1:

                    @pl.when(can_pass(j))
                    def _():
                        pass_on_copy(w, j, c).wait_send()

    for j in range(nz + 1):
        for s in range(sides_x):
            core_copy(j, s).wait_send()
        cross_copy(j).wait_send()

    def end_msg(k, carry):
        msg_copy(k).wait()
        return carry

    with jax.named_scope("end_msg"):
        lax.fori_loop(1, n_all, end_msg, 0)

    total = jnp.zeros((1, LANES), jnp.float32)
    for s in range(n_all):
        total = total + slots[s]
    lane = lax.broadcasted_iota(jnp.int32, (1, LANES), 1)
    place = lax.broadcasted_iota(jnp.int32, (dev_texts, LANES), 0)
    wide = lax.broadcasted_iota(jnp.int32, (dev_texts, LANES), 1)
    picked = jnp.where(wide == dp * dev_texts + place, jnp.broadcast_to(total, wide.shape), 0.0)
    col_own = jnp.sum(picked, axis=1, keepdims=True)
    place_r = lax.broadcasted_iota(jnp.int32, (dev_images, LANES), 0)
    wide_r = lax.broadcasted_iota(jnp.int32, (dev_images, LANES), 1)
    row_own = jnp.zeros((dev_images, 1), jnp.float32)
    for m in range(n_mp):
        theirs = jnp.broadcast_to(slots[dp * n_mp + m], wide_r.shape)
        mine = jnp.logical_and(
            wide_r - pairs == place_r - m * own_images,
            jnp.logical_and(wide_r >= pairs, wide_r < pairs + own_images),
        )
        row_own = row_own + jnp.sum(jnp.where(mine, theirs, 0.0), axis=1, keepdims=True)
    out_ref[0:1, :] = jnp.sum(jnp.where(place_r == wide_r, row_own, 0.0), axis=0, keepdims=True)[:, :dev_images]
    out_ref[1:2, :] = jnp.sum(jnp.where(place == wide, col_own, 0.0), axis=0, keepdims=True)[:, :dev_texts]


def fused(
    n_dp,
    n_mp,
    picture_skip_activations,
    caption_closing_activations,
    normaliser_multipliers,
    widening_matrix,
    contracting_matrix,
    caption_mapping_matrix,
    sharpness_factor,
    score_offset_term,
):
    rows, width = picture_skip_activations.shape
    block, hidden = widening_matrix.shape
    own_rows = rows // n_mp
    nz, sides_x, n_all = n_dp // 2, n_mp // 2, n_dp * n_mp
    dev_texts = caption_closing_activations.shape[0]
    bf16, f32 = jnp.bfloat16, jnp.float32
    vmem = pl.BlockSpec(memory_space=pltpu.VMEM)
    hbm = pl.BlockSpec(memory_space=pl.ANY)
    smem = pl.BlockSpec(memory_space=pltpu.SMEM)
    dma = pltpu.SemaphoreType.DMA
    out = pl.pallas_call(
        functools.partial(fused_kernel, n_dp, n_mp),
        out_shape=jax.ShapeDtypeStruct((2, dev_texts), f32),
        in_specs=[hbm, vmem, vmem, vmem, vmem, hbm, smem, smem],
        out_specs=vmem,
        scratch_shapes=[
            pltpu.VMEM((rows, width), bf16),
            pltpu.VMEM((rows, width), bf16),
            pltpu.VMEM((width, width), bf16),
            pltpu.VMEM((width, hidden), bf16),
            pltpu.VMEM((width, hidden), bf16),
            pltpu.VMEM((rows, hidden), bf16),
            pltpu.VMEM((width, rows), bf16),
            pltpu.VMEM((width, sides_x * own_rows), bf16),
            pltpu.VMEM((width, own_rows), bf16),
            pltpu.VMEM((width, own_rows), bf16),
            pltpu.VMEM((width, own_rows), f32),
            pltpu.VMEM((n_dp, dev_texts, width), bf16),
            pltpu.VMEM((1, LANES), f32),
            pltpu.VMEM((n_all, 1, LANES), f32),
            dma((2,)),
            dma((3, nz, 3)),
            dma((3, nz + 1, 3)),
            dma((3, n_dp, 3)),
            dma((nz + 1, sides_x)),
            dma((nz + 1, sides_x)),
            dma((nz + 1,)),
            dma((nz + 1,)),
            dma((n_all,)),
            dma((n_all,)),
        ],
        compiler_params=pltpu.CompilerParams(
            collective_id=0, has_side_effects=True, vmem_limit_bytes=60 * 1024 * 1024
        ),
    )(
        picture_skip_activations,
        caption_closing_activations,
        normaliser_multipliers,
        widening_matrix,
        contracting_matrix.T,
        caption_mapping_matrix,
        sharpness_factor,
        score_offset_term,
    )
    return out[0], out[1]


def pick(n_dp, n_mp, *args):
    pictures, captions, _, widening = args[:4]
    rows, width = pictures.shape
    pairs = captions.shape[0] * n_dp
    fits = (
        n_dp % 2 == 0
        and n_dp >= 4
        and n_mp == 4
        and widening.shape[0] % 16 == 0
        and rows % (n_mp * PATCHES) == 0
        and width % LANES == 0
        and rows // PATCHES == captions.shape[0]
        and captions.shape[0] % 8 == 0
        and pairs + rows // (n_mp * PATCHES) <= LANES
    )
    return fused(n_dp, n_mp, *args) if fits else on_device(*args)


def solution(mesh):
    return jax.shard_map(
        functools.partial(pick, mesh.shape["dp"], mesh.shape["mp"]),
        mesh=mesh,
        in_specs=(P("dp", None), P("dp", None), P(), P("dp", "mp"), P("mp", "dp"), P(), P(), P()),
        out_specs=(P("dp"), P("dp")),
        check_vma=False,
    )
```
